1024 devices in a mesh: row: 8 (over y), col: 8 (over x_lo, core), rep: 16 (over z, x_hi).
Axes of the slice: x: 8 (x_hi: 2, x_lo: 4; x = x_hi * 4 + x_lo), y: 8, z: 8, core: 2. Of those that a mesh axis runs over, the one named last changes fastest.
Arguments:
- hidden: bfloat16 [2048, 7168], P('rep'), may hold values from -6 to 6
- train_weight: bfloat16 [7168, 16384], P(('rep', 'row'), 'col'), may hold values from -0.0625 to 0.0625
- shard_order: int32 [8, 4, 8], replicated, may hold values from 0 to 7, each once within a row
Outputs:
- served_weight: bfloat16 [7168, 16384], P(None, ('col', 'row'))
- projected: float32 [2048, 16384], P('rep', ('col', 'row'))
The draws below stay inside these ranges and needn't reach their ends.
Inputs may be any that keep to these rules, and one draw needn't show every extreme that they name: Each shard_order[c, k] is a permutation of 0 to 7.
All inputs are finite; a program needn't handle non-finite values.
Results may differ from the reference program's by a relative error of at most 0.001.
Values may be sent and summed in bfloat16 or wider, within the bound.
A program may use at most 32 MiB of HBM per device.

```python
import jax
import jax.numpy as jnp

D = 7168
F = 16384
SUB_BLOCKS = 4
SEQS = 2048
N_ROW = 8
N_COL = 8


def block_scale(rng, shape, cuts, least, high):
    def one(dim, shards_of):
        heights = jax.random.uniform(jax.random.fold_in(jax.random.fold_in(rng, 6), dim), (shards_of,), jnp.float32, least / len(cuts), high / len(cuts))
        return jnp.repeat(jnp.exp(heights), shape[dim] // shards_of).reshape((-1,) + (1,) * (len(shape) - dim - 1))

    loudness = one(*cuts[0])
    for cut in cuts[1:]:
        loudness = loudness * one(*cut)
    return loudness


def centred(key, extent, width, reach, split=(), dtype=jnp.bfloat16):
    drawn = width * jax.random.normal(key, extent, jnp.float32)
    if split:
        drawn = drawn * block_scale(key, extent, split, -0.22, 0.18)
    return jnp.clip(drawn, -reach, reach).astype(dtype)


def setup_inputs(seed: int = 0) -> dict:
    arg_keys = jax.random.split(jax.random.key(seed), 4)
    hidden = centred(arg_keys[0], (SEQS, D), 1.0, 6.0, ((0, 16),))
    train_weight = centred(arg_keys[1], (D, F), D ** -0.5, 0.0625, ((0, 128), (1, 8)))
    shard_order = jax.vmap(lambda own: jax.random.permutation(own, N_ROW))(jax.random.split(arg_keys[2], N_COL * SUB_BLOCKS)).reshape((N_COL, SUB_BLOCKS, N_ROW)).astype(jnp.int32)
    return dict(hidden=hidden, train_weight=train_weight, shard_order=shard_order)


def reference(hidden, train_weight, shard_order):
    block_cols = F // (N_ROW * N_COL)
    sub_cols = block_cols // SUB_BLOCKS
    blocks = train_weight.reshape(D, N_COL, N_ROW, SUB_BLOCKS, sub_cols)
    order = shard_order.astype(jnp.int32)
    pieces = []
    for index in range(SUB_BLOCKS):
        subset = blocks[:, :, :, index, :]
        picks = jnp.broadcast_to(order[:, index, :][None, :, :, None], subset.shape)
        pieces.append(jnp.take_along_axis(subset, picks, axis=2))
    served = jnp.stack(pieces, axis=3).reshape(D, F)
    projected = jnp.dot(hidden, served, preferred_element_type=jnp.float32)
    return served, projected
```

```python
import functools

import jax
import jax.numpy as jnp
from jax import lax
from jax.experimental import pallas as pl
from jax.experimental.pallas import tpu as pltpu
from jax.sharding import PartitionSpec as P

MESH = pl.DeviceIdType.MESH


def handoff(
    sizes, order_ref, hidden_ref, tile_ref, served_ref, projected_ref,
    hidden, tile, pieces, hidden_sem, tile_sem, spread_send, spread_recv, near_send, near_recv, far_send, far_recv,
):
    n_row, n_z, piece_rows, cols, subs = sizes
    half_rows = n_row * piece_rows
    place_rows = 2 * half_rows
    sub_cols = cols // subs
    col = lax.axis_index("col")
    row = lax.axis_index("row")
    rep = lax.axis_index("rep")
    z, half = rep // 2, rep % 2

    lanes = 2 * sub_cols
    load_hidden = pltpu.make_async_copy(hidden_ref, hidden, hidden_sem)
    load_tile = [
        pltpu.make_async_copy(tile_ref.at[:, i * lanes : (i + 1) * lanes], tile.at[i], tile_sem.at[i])
        for i in range(tile.shape[0])
    ]
    for copy in load_tile:
        copy.start()
    load_hidden.start()

    def rep_of(dz, other):
        return lax.rem(z + dz + n_z, n_z) * 2 + (1 - half if other else half)

    def row_of(d):
        return lax.rem(row + d + n_row, n_row)

    spread = [(o, d) for o in (0, 1) for d in (1, 7, 2, 6, 3, 5, 4)]
    spread.insert(7, (1, 0))
    barrier = pltpu.get_barrier_semaphore()
    for o, d in spread:
        pl.semaphore_signal(
            barrier, inc=1, device_id={"row": row_of(d), "rep": rep_of(0, o)}, device_id_type=MESH
        )
    for dz in (1, -1):
        pl.semaphore_signal(barrier, inc=1, device_id={"rep": rep_of(dz, 0)}, device_id_type=MESH)

    for copy in load_tile:
        copy.wait()
    low = lax.broadcasted_iota(jnp.int32, (piece_rows, 2 * sub_cols), 1) < sub_cols
    for s in range(n_row):
        for pair in range(subs // 2):
            first = order_ref[col, 2 * pair, s]
            second = order_ref[col, 2 * pair + 1, s]
            a = tile[first * (subs // 2) + pair]
            b = tile[second * (subs // 2) + pair]
            pieces[s, :, pair * lanes : (pair + 1) * lanes] = jnp.where(low, a, b)

    def piece_at(of_rep, of_row):
        return pl.ds(pl.multiple_of(of_rep * half_rows + of_row * piece_rows, 8), piece_rows)

    def half_at(of_rep):
        return pl.ds(pl.multiple_of(of_rep * half_rows, 8), half_rows)

    served_ref[piece_at(rep, row), :] = pieces[row]
    pl.semaphore_wait(barrier, len(spread) + 2)

    sent = []

    def send(src, at, send_sem, recv_sem, device):
        copy = pltpu.make_async_remote_copy(
            src_ref=src, dst_ref=served_ref.at[at, :], send_sem=send_sem, recv_sem=recv_sem,
            device_id=device, device_id_type=MESH,
        )
        copy.start()
        sent.append(copy)

    def arrived(at, recv_sem, send_sem):
        ref = served_ref.at[at, :]
        pltpu.make_async_remote_copy(
            src_ref=ref, dst_ref=ref, send_sem=send_sem, recv_sem=recv_sem,
            device_id={"rep": rep_of(1, 0)}, device_id_type=MESH,
        ).wait_recv()

    DIRS = ((0, 1), (1, -1))

    def near(o, d):
        at = piece_at(rep_of(0, o), row_of(-d))
        src = pieces.at[row] if (o, d) == (0, 0) else served_ref.at[at, :]
        for way, dz in DIRS:
            send(src, at, near_send.at[way, o, d], near_recv.at[way, o, d], {"rep": rep_of(dz, 0)})

    mine = piece_at(rep, row)
    near(0, 0)
    for o, d in spread:
        send(
            pieces.at[row_of(d)], mine, spread_send.at[o, d], spread_recv.at[o, d],
            {"row": row_of(d), "rep": rep_of(0, o)},
        )
    for o, d in spread:
        arrived(piece_at(rep_of(0, o), row_of(-d)), spread_recv.at[o, d], spread_send.at[o, d])
        near(o, d)

    load_hidden.wait()

    def product(dz):
        place = lax.rem(z + dz + n_z, n_z)
        at = pl.ds(pl.multiple_of(place * place_rows, 128), place_rows)
        return jnp.dot(hidden[:, at], served_ref[at, :], preferred_element_type=jnp.float32)

    projected_ref[...] = product(0)
    last = n_z // 2
    for step in range(1, last):
        for o in (0, 1):
            for way, dz in DIRS:
                at = half_at(rep_of(-dz * step, o))
                if step == 1:
                    for d in range(n_row):
                        arrived(
                            piece_at(rep_of(-dz, o), row_of(-d)), near_recv.at[way, o, d], near_send.at[way, o, d]
                        )
                else:
                    arrived(at, far_recv.at[way, step - 2, o], far_send.at[way, step - 2, o])
                if step < last - 1 or o == way:
                    send(
                        served_ref.at[at, :], at, far_send.at[way, step - 1, o], far_recv.at[way, step - 1, o],
                        {"rep": rep_of(dz, 0)},
                    )
        projected_ref[...] += product(step)
        projected_ref[...] += product(-step)
    for way, dz in DIRS:
        arrived(half_at(rep_of(-dz * last, way)), far_recv.at[way, last - 2, way], far_send.at[way, last - 2, way])
    projected_ref[...] += product(last)
    for copy in sent:
        copy.wait_send()


def solution(mesh):
    n_row, n_rep = mesh.shape["row"], mesh.shape["rep"]

    def shards(hidden, train_weight, shard_order):
        piece_rows, tile_cols = train_weight.shape
        cols = tile_cols // n_row
        subs = shard_order.shape[1]
        n_z = n_rep // 2
        depth = hidden.shape[1]
        dma = pltpu.SemaphoreType.DMA
        return pl.pallas_call(
            functools.partial(handoff, (n_row, n_z, piece_rows, cols, subs)),
            out_shape=(
                jax.ShapeDtypeStruct((depth, cols), jnp.bfloat16),
                jax.ShapeDtypeStruct((hidden.shape[0], cols), jnp.float32),
            ),
            in_specs=[
                pl.BlockSpec(memory_space=pltpu.SMEM),
                pl.BlockSpec(memory_space=pl.ANY),
                pl.BlockSpec(memory_space=pl.ANY),
            ],
            out_specs=[pl.BlockSpec(memory_space=pltpu.VMEM)] * 2,
            scratch_shapes=[
                pltpu.VMEM(hidden.shape, jnp.bfloat16),
                pltpu.VMEM((tile_cols * subs // (2 * cols), piece_rows, 2 * cols // subs), jnp.bfloat16),
                pltpu.VMEM((n_row, piece_rows, cols), jnp.bfloat16),
                dma,
                dma((tile_cols * subs // (2 * cols),)),
                dma((2, n_row)),
                dma((2, n_row)),
                dma((2, 2, n_row)),
                dma((2, 2, n_row)),
                dma((2, n_z // 2 - 1, 2)),
                dma((2, n_z // 2 - 1, 2)),
            ],
            compiler_params=pltpu.CompilerParams(collective_id=0, has_side_effects=True),
            name="handoff",
        )(shard_order, hidden, train_weight)

    return jax.shard_map(
        shards,
        mesh=mesh,
        in_specs=(P("rep", None), P(("rep", "row"), "col"), P()),
        out_specs=(P(None, ("col", "row")), P("rep", ("col", "row"))),
        check_vma=False,
    )
```

```python
import functools

import jax
import jax.numpy as jnp
from jax import lax
from jax.experimental import pallas as pl
from jax.experimental.pallas import tpu as pltpu
from jax.sharding import PartitionSpec as P

MESH = pl.DeviceIdType.MESH
UP, DOWN = 0, 1
STEP = {UP: 1, DOWN: -1}


def handoff(
    sizes, order_hbm, hidden_hbm, tile_hbm, served, projected,
    order, hidden, tile, pieces, relayed, local_sem, tile_sem, ready,
    row_send, row_recv, out_send, out_recv, on_send, on_recv, z_send, z_recv,
):
    n, n_x, piece_rows, cols, subs = sizes
    half_rows = n * piece_rows
    place_rows = 2 * half_rows
    lanes = 2 * cols // subs
    x_los = n_x // 2
    col = lax.axis_index("col")
    row = lax.axis_index("row")
    rep = lax.axis_index("rep")
    z, half = rep // 2, rep % 2
    x = half * x_los + col // 2

    load_order = pltpu.make_async_copy(order_hbm, order, local_sem.at[0])
    load_hidden = pltpu.make_async_copy(hidden_hbm, hidden, local_sem.at[1])
    load_tile = [
        pltpu.make_async_copy(tile_hbm.at[:, i * lanes : (i + 1) * lanes], tile.at[i], tile_sem.at[i])
        for i in range(tile.shape[0])
    ]
    load_order.start()
    for copy in load_tile:
        copy.start()
    load_hidden.start()

    def row_of(d):
        return (row + d + n) % n

    def rep_of(e, other):
        return (z + e + n) % n * 2 + (half + other) % 2

    def x_device(w):
        far = (x + 2 * w + n_x) % n_x
        return {"col": far % x_los * 2 + col % 2, "rep": z * 2 + far // x_los}

    def z_device(e):
        return {"rep": rep_of(e, 0)}

    def side(d):
        return 1 - 2 * (d // (n // 2))

    barrier = pltpu.get_barrier_semaphore()

    def greet(device):
        pl.semaphore_signal(barrier, inc=1, device_id=device, device_id_type=MESH)

    for d in range(1, n):
        greet({"row": row_of(d)})
    for w in (1, -1):
        greet(x_device(w))

    @pl.when(z < n - 1)
    def _():
        greet(z_device(1))

    @pl.when(z == 0)
    def _():
        greet(z_device(-1))

    load_order.wait()
    for copy in load_tile:
        copy.wait()
    low = lax.broadcasted_iota(jnp.int32, (piece_rows, lanes), 1) < lanes // 2
    for s in range(n):
        for pair in range(subs // 2):
            a = tile[order[col, 2 * pair, s] * (subs // 2) + pair]
            b = tile[order[col, 2 * pair + 1, s] * (subs // 2) + pair]
            pieces[s, :, pair * lanes : (pair + 1) * lanes] = jnp.where(low, a, b)

    def piece_at(of_rep, of_row):
        return pl.ds(pl.multiple_of(of_rep * half_rows + of_row * piece_rows, 8), piece_rows)

    served[piece_at(rep, row), :] = pieces[row]
    pl.semaphore_wait(barrier, n + 1 + (z + n - 2) // (n - 1) + z // (n - 1))

    @pl.when(z > 0)
    def _():
        pl.semaphore_signal(ready.at[UP], inc=1, device_id=z_device(-1), device_id_type=MESH)

    @pl.when(z == n - 1)
    def _():
        pl.semaphore_signal(ready.at[DOWN], inc=1, device_id=z_device(1), device_id_type=MESH)

    def copy_of(src, dst, send_sem, recv_sem, device):
        return pltpu.make_async_remote_copy(
            src_ref=src, dst_ref=dst, send_sem=send_sem, recv_sem=recv_sem, device_id=device, device_id_type=MESH
        )

    def await_piece(recv_sem, send_sem):
        copy_of(pieces.at[0], relayed.at[0], send_sem, recv_sem, z_device(1)).wait_recv()

    def served_piece(e, other, d):
        return served.at[piece_at(rep_of(e, other), row_of(-d)), :]

    mine = served.at[piece_at(rep, row), :]

    def nth(i):
        return (i % 2 * ((i + 1) // 2) + (1 - i % 2) * (n - i // 2)) % n

    def each(body):
        lax.fori_loop(0, n, lambda i, c: (body(nth(i)), c)[1], 0)

    for i in range(1, n):
        d = nth(i)
        copy_of(pieces.at[row_of(d)], mine, row_send.at[d], row_recv.at[d], {"row": row_of(d)}).start()

    def z_copy(way, step, other, d):
        piece = served_piece(-STEP[way] * (step - 1), other, d)
        at = (way, step - 1, other, d)
        return copy_of(piece, piece, z_send.at[at], z_recv.at[at], z_device(STEP[way]))

    def own(ways, fresh):
        def go(d):
            for way in ways:
                z_copy(way, 1, 0, d).start()
            if fresh:
                piece = served_piece(0, 0, d)
                copy_of(piece, relayed.at[d], out_send.at[d], out_recv.at[d], x_device(side(d))).start()

        def body(i, c):
            d = nth(i)
            if fresh:
                await_piece(row_recv.at[d], row_send.at[d])
            go(d)
            return c

        go(0)
        lax.fori_loop(1, n, body, 0)

    def relay(d):
        await_piece(out_recv.at[d], out_send.at[d])
        w = side(d)
        origin = (x - 2 * w + n_x) % n_x // x_los
        at = piece_at(z * 2 + origin, row_of(-d))
        copy_of(relayed.at[d], served.at[at, :], on_send.at[d], on_recv.at[d], x_device(w)).start()

    def others(ways, wait):
        def body(d):
            if wait:
                await_piece(on_recv.at[d], on_send.at[d])
            for way in ways:
                z_copy(way, 1, 1, d).start()

        each(body)

    def z_await(way, step, other, d):
        await_piece(z_recv.at[way, step - 1, other, d], z_send.at[way, step - 1, other, d])

    def z_pass(way, step, other, d):
        z_await(way, step, other, d)
        z_copy(way, step + 1, other, d).start()

    def pass_on(*moves):
        def body(d):
            for move in moves:
                z_pass(*move, d)

        each(body)

    BOTH = (DOWN, UP)

    far_down = (z > 0) & (z < 5)
    far_up = (z > 2) & (z < 7)

    def pass_third(other):
        def body(d):
            @pl.when(far_down)
            def _():
                z_pass(DOWN, 3, other, d)

            @pl.when(far_up)
            def _():
                z_pass(UP, 3, other, d)

        each(body)

    @pl.when(z == 0)
    def _():
        pl.semaphore_wait(ready.at[UP], 1)
        own((UP,), True)
        each(relay)
        others((UP,), True)
        pl.semaphore_wait(ready.at[DOWN], 1)
        own((DOWN,), False)
        pass_on((DOWN, 1, 0))
        others((DOWN,), False)
        pass_on((DOWN, 1, 1))
        pass_on((DOWN, 2, 0))
        pass_on((UP, 1, 0))
        pass_on((UP, 2, 0))
        pass_on((DOWN, 2, 1))
        pass_on((UP, 1, 1))
        pass_on((UP, 2, 1))

    @pl.when(z > 0)
    def _():
        @pl.when(z == n - 1)
        def _():
            own(BOTH, True)

        @pl.when(z < n - 1)
        def _():
            own((DOWN,), True)
            pl.semaphore_wait(ready.at[UP], 1)
            own((UP,), False)

        def body(d):
            z_pass(DOWN, 1, 0, d)
            relay(d)
            z_pass(UP, 1, 0, d)

        each(body)

        @pl.when(z == 1)
        def _():
            pass_on((DOWN, 2, 0))
            others(BOTH, True)
            pass_on((DOWN, 1, 1), (UP, 1, 1))
            pass_third(0)
            pass_on((DOWN, 2, 1), (UP, 2, 0))
            pass_third(1)
            pass_on((UP, 2, 1))

        @pl.when(z > 1)
        def _():
            pass_on((DOWN, 2, 0), (UP, 2, 0))
            others(BOTH, True)
            pass_on((DOWN, 1, 1), (UP, 1, 1))
            pass_third(0)
            pass_on((DOWN, 2, 1), (UP, 2, 1))
            pass_third(1)

    load_hidden.wait()

    def product(e):
        at = pl.ds(pl.multiple_of((z + e + n) % n * place_rows, 128), place_rows)
        return jnp.dot(hidden[:, at], served[at, :], preferred_element_type=jnp.float32)

    def sent(sem):
        copy_of(pieces.at[0], relayed.at[0], sem, sem, z_device(1)).wait_send()

    def sent_before(d):
        sent(out_send.at[d])
        sent(on_send.at[d])
        for way in BOTH:
            for other in (0, 1):
                sent(z_send.at[way, 0, other, d])

    def sent_last(d):
        for way, far in ((DOWN, far_down), (UP, far_up)):
            for other in (0, 1):
                sent(z_send.at[way, 1, other, d])
                sent(z_send.at[way, 2, other, d])

                @pl.when(far)
                def _():
                    sent(z_send.at[way, 3, other, d])

    def third_here(way, far):
        @pl.when(jnp.logical_not(far))
        def _():
            for other in (0, 1):
                each(functools.partial(z_await, way, 3, other))

    projected[...] = product(0)

    def add(e, c):
        projected[...] += product(e)
        return c

    lax.fori_loop(1, 3, lambda e, c: add(n - e, add(e, c)), 0)
    lax.fori_loop(1, n, lambda d, c: (sent(row_send.at[d]), c)[1], 0)
    each(sent_before)
    third_here(DOWN, far_down)
    projected[...] += product(3)

    @pl.when(z < n // 2)
    def _():
        for other in (0, 1):
            each(functools.partial(z_await, DOWN, 4, other))

    @pl.when(z >= n // 2)
    def _():
        for other in (0, 1):
            each(functools.partial(z_await, UP, 4, other))

    projected[...] += product(4)
    third_here(UP, far_up)
    projected[...] += product(-3)
    each(sent_last)


def solution(mesh):
    n_row, n_col, n_rep = mesh.shape["row"], mesh.shape["col"], mesh.shape["rep"]

    def shards(hidden, train_weight, shard_order):
        piece_rows, tile_cols = train_weight.shape
        cols = tile_cols // n_row
        subs = shard_order.shape[1]
        depth = hidden.shape[1]
        tiles = n_row * subs // 2
        dma = pltpu.SemaphoreType.DMA
        one = dma((n_row,))
        ring = dma((2, 4, 2, n_row))
        return pl.pallas_call(
            functools.partial(handoff, (n_row, n_col, piece_rows, cols, subs)),
            out_shape=(
                jax.ShapeDtypeStruct((depth, cols), jnp.bfloat16),
                jax.ShapeDtypeStruct((hidden.shape[0], cols), jnp.float32),
            ),
            in_specs=[pl.BlockSpec(memory_space=pltpu.HBM)] * 3,
            out_specs=[pl.BlockSpec(memory_space=pltpu.VMEM)] * 2,
            scratch_shapes=[
                pltpu.SMEM(shard_order.shape, jnp.int32),
                pltpu.VMEM(hidden.shape, jnp.bfloat16),
                pltpu.VMEM((tiles, piece_rows, tile_cols // tiles), jnp.bfloat16),
                pltpu.VMEM((n_row, piece_rows, cols), jnp.bfloat16),
                pltpu.VMEM((n_row, piece_rows, cols), jnp.bfloat16),
                dma((2,)),
                dma((tiles,)),
                pltpu.SemaphoreType.REGULAR((2,)),
                one, one, one, one, one, one, ring, ring,
            ],
            compiler_params=pltpu.CompilerParams(
                collective_id=0, has_side_effects=True, vmem_limit_bytes=16 * 1024 * 1024
            ),
            name="handoff",
        )(*[pltpu.with_memory_space_constraint(a, pltpu.HBM) for a in (shard_order, hidden, train_weight)])

    return jax.shard_map(
        shards,
        mesh=mesh,
        in_specs=(P("rep", None), P(("rep", "row"), "col"), P()),
        out_specs=(P(None, ("col", "row")), P("rep", ("col", "row"))),
        check_vma=False,
    )
```

```python
import functools

import jax
import jax.numpy as jnp
from jax import lax
from jax.experimental import pallas as pl
from jax.experimental.pallas import tpu as pltpu
from jax.sharding import PartitionSpec as P

MESH = pl.DeviceIdType.MESH
UP, DOWN = 0, 1
STEP = {UP: 1, DOWN: -1}


def handoff(
    sizes, order_hbm, hidden_hbm, tile_hbm, served, projected,
    order, hidden, tile, pieces, relayed, local_sem, tile_sem, ready,
    row_recv, out_recv, on_recv, z_recv, sent,
):
    n, n_x, piece_rows, cols, subs = sizes
    half_rows = n * piece_rows
    place_rows = 2 * half_rows
    lanes = 2 * cols // subs
    x_los = n_x // 2
    col = lax.axis_index("col")
    row = lax.axis_index("row")
    rep = lax.axis_index("rep")
    z, half = rep // 2, rep % 2
    x = half * x_los + col // 2

    load_order = pltpu.make_async_copy(order_hbm, order, local_sem.at[0])
    load_hidden = pltpu.make_async_copy(hidden_hbm, hidden, local_sem.at[1])
    load_tile = [
        pltpu.make_async_copy(tile_hbm.at[:, i * lanes : (i + 1) * lanes], tile.at[i], tile_sem)
        for i in range(tile.shape[0])
    ]
    load_order.start()
    for copy in load_tile:
        copy.start()
    load_hidden.start()

    def row_of(d):
        return (row + d + n) % n

    def rep_of(e, other):
        return (z + e + n) % n * 2 + (half + other) % 2

    def x_device(w):
        far = (x + 2 * w + n_x) % n_x
        return {"col": far % x_los * 2 + col % 2, "rep": z * 2 + far // x_los}

    def z_device(e):
        return {"rep": rep_of(e, 0)}

    def side(d):
        return 1 - 2 * (d // (n // 2))

    barrier = pltpu.get_barrier_semaphore()

    def greet(device):
        pl.semaphore_signal(barrier, inc=1, device_id=device, device_id_type=MESH)

    for d in range(1, n):
        greet({"row": row_of(d)})
    for w in (1, -1):
        greet(x_device(w))

    @pl.when(z < n - 1)
    def _():
        greet(z_device(1))

    @pl.when(z == 0)
    def _():
        greet(z_device(-1))

    load_order.wait()
    pltpu.make_async_copy(tile, tile, tile_sem).wait()
    low = lax.broadcasted_iota(jnp.int32, (piece_rows, lanes), 1) < lanes // 2
    for s in range(n):
        for pair in range(subs // 2):
            a = tile[order[col, 2 * pair, s] * (subs // 2) + pair]
            b = tile[order[col, 2 * pair + 1, s] * (subs // 2) + pair]
            pieces[s, :, pair * lanes : (pair + 1) * lanes] = jnp.where(low, a, b)

    def piece_at(of_rep, of_row):
        return pl.ds(pl.multiple_of(of_rep * half_rows + of_row * piece_rows, 8), piece_rows)

    served[piece_at(rep, row), :] = pieces[row]
    pl.semaphore_wait(barrier, n + 1 + (z + n - 2) // (n - 1) + z // (n - 1))

    @pl.when(z > 0)
    def _():
        pl.semaphore_signal(ready.at[UP], inc=1, device_id=z_device(-1), device_id_type=MESH)

    @pl.when(z == n - 1)
    def _():
        pl.semaphore_signal(ready.at[DOWN], inc=1, device_id=z_device(1), device_id_type=MESH)

    def copy_of(src, dst, send_sem, recv_sem, device):
        return pltpu.make_async_remote_copy(
            src_ref=src, dst_ref=dst, send_sem=send_sem, recv_sem=recv_sem, device_id=device, device_id_type=MESH
        )

    def await_piece(recv_sem, send_sem):
        copy_of(pieces.at[0], relayed.at[0], send_sem, recv_sem, z_device(1)).wait_recv()

    def served_piece(e, other, d):
        return served.at[piece_at(rep_of(e, other), row_of(-d)), :]

    mine = served.at[piece_at(rep, row), :]

    def nth(i):
        return (i % 2 * ((i + 1) // 2) + (1 - i % 2) * (n - i // 2)) % n

    def each(body):
        lax.fori_loop(0, n, lambda i, c: (body(nth(i)), c)[1], 0)

    for i in range(1, n):
        d = nth(i)
        copy_of(pieces.at[row_of(d)], mine, sent.at[0], row_recv.at[d], {"row": row_of(d)}).start()

    def z_sem(way, step, other, d):
        return z_recv.at[0 if step == n // 2 else 3 * way + step, other, d]

    def z_copy(way, step, other, d):
        piece = served_piece(-STEP[way] * (step - 1), other, d)
        sem = sent.at[1 + way] if step == n // 2 else sent.at[0]
        return copy_of(piece, piece, sem, z_sem(way, step, other, d), z_device(STEP[way]))

    def own(ways, fresh):
        def go(d):
            for way in ways:
                z_copy(way, 1, 0, d).start()
            if fresh:
                piece = served_piece(0, 0, d)
                copy_of(piece, relayed.at[d], sent.at[0], out_recv.at[d], x_device(side(d))).start()

        def body(i, c):
            d = nth(i)
            if fresh:
                await_piece(row_recv.at[d], sent.at[0])
            go(d)
            return c

        go(0)
        lax.fori_loop(1, n, body, 0)

    def relay(d):
        await_piece(out_recv.at[d], sent.at[0])
        w = side(d)
        origin = (x - 2 * w + n_x) % n_x // x_los
        at = piece_at(z * 2 + origin, row_of(-d))
        copy_of(relayed.at[d], served.at[at, :], sent.at[0], on_recv.at[d], x_device(w)).start()

    def others(ways, wait):
        def body(d):
            if wait:
                await_piece(on_recv.at[d], sent.at[0])
            for way in ways:
                z_copy(way, 1, 1, d).start()

        each(body)

    def z_await(way, step, other, d):
        await_piece(z_sem(way, step, other, d), sent.at[0])

    def z_pass(way, step, other, d):
        z_await(way, step, other, d)
        z_copy(way, step + 1, other, d).start()

    def pass_on(*moves):
        def body(d):
            for move in moves:
                z_pass(*move, d)

        each(body)

    BOTH = (DOWN, UP)

    far_down = (z > 0) & (z < 5)
    far_up = (z > 2) & (z < 7)

    def pass_third(other):
        def body(d):
            @pl.when(far_down)
            def _():
                z_pass(DOWN, 3, other, d)

            @pl.when(far_up)
            def _():
                z_pass(UP, 3, other, d)

        each(body)

    @pl.when(z == 0)
    def _():
        pl.semaphore_wait(ready.at[UP], 1)
        own((UP,), True)
        each(relay)
        others((UP,), True)
        pl.semaphore_wait(ready.at[DOWN], 1)
        own((DOWN,), False)
        pass_on((DOWN, 1, 0))
        others((DOWN,), False)
        pass_on((DOWN, 1, 1))
        pass_on((DOWN, 2, 0))
        pass_on((UP, 1, 0))
        pass_on((UP, 2, 0))
        pass_on((DOWN, 2, 1))
        pass_on((UP, 1, 1))
        pass_on((UP, 2, 1))

    @pl.when(z > 0)
    def _():
        @pl.when(z == n - 1)
        def _():
            own(BOTH, True)

        @pl.when(z < n - 1)
        def _():
            own((DOWN,), True)
            pl.semaphore_wait(ready.at[UP], 1)
            own((UP,), False)

        def body(d):
            z_pass(DOWN, 1, 0, d)
            relay(d)
            z_pass(UP, 1, 0, d)

        each(body)

        @pl.when(z == 1)
        def _():
            pass_on((DOWN, 2, 0))
            others(BOTH, True)
            pass_on((DOWN, 1, 1), (UP, 1, 1))
            pass_third(0)
            pass_on((DOWN, 2, 1), (UP, 2, 0))
            pass_third(1)
            pass_on((UP, 2, 1))

        @pl.when(z > 1)
        def _():
            pass_on((DOWN, 2, 0), (UP, 2, 0))
            others(BOTH, True)
            pass_on((DOWN, 1, 1), (UP, 1, 1))
            pass_third(0)
            pass_on((DOWN, 2, 1), (UP, 2, 1))
            pass_third(1)

    load_hidden.wait()

    def product(e):
        at = pl.ds(pl.multiple_of((z + e + n) % n * place_rows, 128), place_rows)
        return jnp.dot(hidden[:, at], served[at, :], preferred_element_type=jnp.float32)

    def sent_pieces(sem, count):
        ref = served.at[pl.ds(0, count * piece_rows), :]
        copy_of(ref, ref, sem, sem, z_device(1)).wait_send()

    def all_sent():
        rest = n - 0
        sent_pieces(sent.at[0], 3 * n - 1 + 6 * (n + rest))
        for way, far in ((DOWN, far_down), (UP, far_up)):

            @pl.when(far)
            def _():
                sent_pieces(sent.at[1 + way], n + rest)

    def third_here(way, far):
        @pl.when(jnp.logical_not(far))
        def _():
            for other in (0, 1):
                each(functools.partial(z_await, way, 3, other))

    projected[...] = product(0)

    def add(e, c):
        projected[...] += product(e)
        return c

    lax.fori_loop(1, 3, lambda e, c: add(n - e, add(e, c)), 0)
    third_here(DOWN, far_down)
    projected[...] += product(3)

    @pl.when(z < n // 2)
    def _():
        for other in (0, 1):
            each(functools.partial(z_await, DOWN, 4, other))

    @pl.when(z >= n // 2)
    def _():
        for other in (0, 1):
            each(functools.partial(z_await, UP, 4, other))

    projected[...] += product(4)
    third_here(UP, far_up)
    projected[...] += product(-3)
    all_sent()


def solution(mesh):
    n_row, n_col, n_rep = mesh.shape["row"], mesh.shape["col"], mesh.shape["rep"]

    def shards(hidden, train_weight, shard_order):
        piece_rows, tile_cols = train_weight.shape
        cols = tile_cols // n_row
        subs = shard_order.shape[1]
        depth = hidden.shape[1]
        tiles = n_row * subs // 2
        dma = pltpu.SemaphoreType.DMA
        one = dma((n_row,))
        ring = dma((7, 2, n_row))
        return pl.pallas_call(
            functools.partial(handoff, (n_row, n_col, piece_rows, cols, subs)),
            out_shape=(
                jax.ShapeDtypeStruct((depth, cols), jnp.bfloat16),
                jax.ShapeDtypeStruct((hidden.shape[0], cols), jnp.float32),
            ),
            in_specs=[pl.BlockSpec(memory_space=pltpu.HBM)] * 3,
            out_specs=[pl.BlockSpec(memory_space=pltpu.VMEM)] * 2,
            scratch_shapes=[
                pltpu.SMEM(shard_order.shape, jnp.int32),
                pltpu.VMEM(hidden.shape, jnp.bfloat16),
                pltpu.VMEM((tiles, piece_rows, tile_cols // tiles), jnp.bfloat16),
                pltpu.VMEM((n_row, piece_rows, cols), jnp.bfloat16),
                pltpu.VMEM((n_row, piece_rows, cols), jnp.bfloat16),
                dma((2,)),
                dma,
                pltpu.SemaphoreType.REGULAR((2,)),
                one, one, one, ring, dma((4,)),
            ],
            compiler_params=pltpu.CompilerParams(
                collective_id=0, has_side_effects=True, vmem_limit_bytes=16 * 1024 * 1024
            ),
            name="handoff",
        )(*[pltpu.with_memory_space_constraint(a, pltpu.HBM) for a in (shard_order, hidden, train_weight)])

    return jax.shard_map(
        shards,
        mesh=mesh,
        in_specs=(P("rep", None), P(("rep", "row"), "col"), P()),
        out_specs=(P(None, ("col", "row")), P("rep", ("col", "row"))),
        check_vma=False,
    )
```

```python
import functools

import jax
import jax.numpy as jnp
from jax import lax
from jax.experimental import pallas as pl
from jax.experimental.pallas import tpu as pltpu
from jax.sharding import PartitionSpec as P

MESH = pl.DeviceIdType.MESH
UP, DOWN = 0, 1
STEP = {UP: 1, DOWN: -1}


def handoff(
    sizes, order_hbm, hidden_hbm, tile_hbm, served, projected,
    order, hidden, tile, pieces, relayed, local_sem, tile_sem, ready,
    row_recv, out_recv, on_recv, z_recv, sent,
):
    n, n_x, piece_rows, cols, subs = sizes
    half_rows = n * piece_rows
    place_rows = 2 * half_rows
    lanes = 2 * cols // subs
    x_los = n_x // 2
    col = lax.axis_index("col")
    row = lax.axis_index("row")
    rep = lax.axis_index("rep")
    z, half = rep // 2, rep % 2
    x = half * x_los + col // 2

    load_order = pltpu.make_async_copy(order_hbm, order, local_sem.at[0])
    load_hidden = pltpu.make_async_copy(hidden_hbm, hidden, local_sem.at[1])
    load_tile = [
        pltpu.make_async_copy(tile_hbm.at[:, i * lanes : (i + 1) * lanes], tile.at[i], tile_sem)
        for i in range(tile.shape[0])
    ]
    load_order.start()
    for copy in load_tile:
        copy.start()
    load_hidden.start()

    def row_of(d):
        return (row + d + n) % n

    def rep_of(e, other):
        return (z + e + n) % n * 2 + (half + other) % 2

    def x_device(w):
        far = (x + 2 * w + n_x) % n_x
        return {"col": far % x_los * 2 + col % 2, "rep": z * 2 + far // x_los}

    def z_device(e):
        return {"rep": rep_of(e, 0)}

    def side(d):
        return 1 - 2 * (d // (n // 2))

    barrier = pltpu.get_barrier_semaphore()

    def greet(device):
        pl.semaphore_signal(barrier, inc=1, device_id=device, device_id_type=MESH)

    for d in range(1, n):
        greet({"row": row_of(d)})
    for w in (1, -1):
        greet(x_device(w))

    @pl.when(z < n - 1)
    def _():
        greet(z_device(1))

    @pl.when(z == 0)
    def _():
        greet(z_device(-1))

    load_order.wait()
    pltpu.make_async_copy(tile, tile, tile_sem).wait()
    low = lax.broadcasted_iota(jnp.int32, (piece_rows, lanes), 1) < lanes // 2
    for s in range(n):
        for pair in range(subs // 2):
            a = tile[order[col, 2 * pair, s] * (subs // 2) + pair]
            b = tile[order[col, 2 * pair + 1, s] * (subs // 2) + pair]
            pieces[s, :, pair * lanes : (pair + 1) * lanes] = jnp.where(low, a, b)

    def piece_at(of_rep, of_row):
        return pl.ds(pl.multiple_of(of_rep * half_rows + of_row * piece_rows, 8), piece_rows)

    served[piece_at(rep, row), :] = pieces[row]
    pl.semaphore_wait(barrier, n + 1 + (z + n - 2) // (n - 1) + z // (n - 1))

    @pl.when(z > 0)
    def _():
        pl.semaphore_signal(ready.at[UP], inc=1, device_id=z_device(-1), device_id_type=MESH)

    @pl.when(z == n - 1)
    def _():
        pl.semaphore_signal(ready.at[DOWN], inc=1, device_id=z_device(1), device_id_type=MESH)

    def copy_of(src, dst, send_sem, recv_sem, device):
        return pltpu.make_async_remote_copy(
            src_ref=src, dst_ref=dst, send_sem=send_sem, recv_sem=recv_sem, device_id=device, device_id_type=MESH
        )

    def await_piece(recv_sem, send_sem):
        copy_of(pieces.at[0], relayed.at[0], send_sem, recv_sem, z_device(1)).wait_recv()

    def served_piece(e, other, d):
        return served.at[piece_at(rep_of(e, other), row_of(-d)), :]

    mine = served.at[piece_at(rep, row), :]

    def nth(i):
        return (i % 2 * ((i + 1) // 2) + (1 - i % 2) * (n - i // 2)) % n

    def each(body):
        lax.fori_loop(0, n, lambda i, c: (body(nth(i)), c)[1], 0)

    for i in range(1, n):
        d = nth(i)
        copy_of(pieces.at[row_of(d)], mine, sent.at[0], row_recv.at[d], {"row": row_of(d)}).start()

    def z_sem(way, step, other, d):
        return z_recv.at[0 if step == n // 2 else 3 * way + step, other, d]

    def z_copy(way, step, other, d):
        piece = served_piece(-STEP[way] * (step - 1), other, d)
        sem = sent.at[1 + way] if step == n // 2 else sent.at[0]
        return copy_of(piece, piece, sem, z_sem(way, step, other, d), z_device(STEP[way]))

    def own(ways, fresh):
        def go(d):
            for way in ways:
                z_copy(way, 1, 0, d).start()
            if fresh:
                piece = served_piece(0, 0, d)
                copy_of(piece, relayed.at[d], sent.at[0], out_recv.at[d], x_device(side(d))).start()

        def body(i, c):
            d = nth(i)
            if fresh:
                await_piece(row_recv.at[d], sent.at[0])
            go(d)
            return c

        go(0)
        lax.fori_loop(1, n, body, 0)

    def relay(d):
        await_piece(out_recv.at[d], sent.at[0])
        w = side(d)
        origin = (x - 2 * w + n_x) % n_x // x_los
        at = piece_at(z * 2 + origin, row_of(-d))
        copy_of(relayed.at[d], served.at[at, :], sent.at[0], on_recv.at[d], x_device(w)).start()

    def others(ways, wait):
        def body(d):
            if wait:
                await_piece(on_recv.at[d], sent.at[0])
            for way in ways:
                z_copy(way, 1, 1, d).start()

        each(body)

    def z_await(way, step, other, d):
        await_piece(z_sem(way, step, other, d), sent.at[0])

    def z_pass(way, step, other, d):
        z_await(way, step, other, d)
        z_copy(way, step + 1, other, d).start()

    def pass_on(*moves):
        def body(d):
            for move in moves:
                z_pass(*move, d)

        each(body)

    BOTH = (DOWN, UP)

    far_down = (z > 0) & (z < 5)
    far_up = (z > 2) & (z < 7)

    def pass_third(other):
        def body(d):
            @pl.when(far_down)
            def _():
                z_pass(DOWN, 3, other, d)

            @pl.when(far_up)
            def _():
                z_pass(UP, 3, other, d)

        each(body)

    @pl.when(z == 0)
    def _():
        pl.semaphore_wait(ready.at[UP], 1)
        own((UP,), True)
        each(relay)
        others((UP,), True)
        pl.semaphore_wait(ready.at[DOWN], 1)
        own((DOWN,), False)
        pass_on((DOWN, 1, 0))
        others((DOWN,), False)
        pass_on((DOWN, 1, 1))
        pass_on((DOWN, 2, 0))
        pass_on((UP, 1, 0))
        pass_on((UP, 2, 0))
        pass_on((DOWN, 2, 1))
        pass_on((UP, 1, 1))
        pass_on((UP, 2, 1))

    @pl.when(z > 0)
    def _():
        @pl.when(z == n - 1)
        def _():
            own(BOTH, True)

        @pl.when(z < n - 1)
        def _():
            own((DOWN,), True)
            pl.semaphore_wait(ready.at[UP], 1)
            own((UP,), False)

        def body(d):
            z_pass(DOWN, 1, 0, d)
            relay(d)
            z_pass(UP, 1, 0, d)

        each(body)

        @pl.when(z == 1)
        def _():
            pass_on((DOWN, 2, 0))
            others(BOTH, True)
            pass_on((DOWN, 1, 1), (UP, 1, 1))
            pass_third(0)
            pass_on((DOWN, 2, 1), (UP, 2, 0))
            pass_third(1)
            pass_on((UP, 2, 1))

        @pl.when(z > 1)
        def _():
            pass_on((DOWN, 2, 0), (UP, 2, 0))
            others(BOTH, True)
            pass_on((DOWN, 1, 1), (UP, 1, 1))
            pass_third(0)
            pass_on((DOWN, 2, 1), (UP, 2, 1))
            pass_third(1)

    load_hidden.wait()

    def product(e):
        at = pl.ds(pl.multiple_of((z + e + n) % n * place_rows, 128), place_rows)
        return jnp.dot(hidden[:, at], served[at, :], preferred_element_type=jnp.float32)

    def sent_pieces(sem, count):
        ref = served.at[pl.ds(0, count * piece_rows), :]
        copy_of(ref, ref, sem, sem, z_device(1)).wait_send()

    def all_sent():
        rest = n - 0
        sent_pieces(sent.at[0], 3 * n - 1 + 6 * (n + rest))
        for way, far in ((DOWN, far_down), (UP, far_up)):

            @pl.when(far)
            def _():
                sent_pieces(sent.at[1 + way], n + rest)

    def third_here(way, far):
        @pl.when(jnp.logical_not(far))
        def _():
            for other in (0, 1):
                each(functools.partial(z_await, way, 3, other))

    projected[...] = product(0)

    def add(e, c):
        projected[...] += product(e)
        return c

    lax.fori_loop(1, 3, lambda e, c: add(n - e, add(e, c)), 0)
    third_here(DOWN, far_down)
    projected[...] += product(3)

    @pl.when(z < n // 2)
    def _():
        for other in (0, 1):
            each(functools.partial(z_await, DOWN, 4, other))

    @pl.when(z >= n // 2)
    def _():
        for other in (0, 1):
            each(functools.partial(z_await, UP, 4, other))

    projected[...] += product(4)
    third_here(UP, far_up)
    projected[...] += product(-3)
    all_sent()


def put_out(chunks, served, projected, served_out, projected_out, sem):
    rows = served.shape[0] // chunks
    copies = [pltpu.make_async_copy(projected, projected_out, sem.at[chunks])] + [
        pltpu.make_async_copy(served.at[pl.ds(i * rows, rows), :], served_out.at[pl.ds(i * rows, rows), :], sem.at[i])
        for i in range(chunks)
    ]
    for copy in copies:
        copy.start()
    for copy in copies:
        copy.wait()


def solution(mesh):
    n_row, n_col, n_rep = mesh.shape["row"], mesh.shape["col"], mesh.shape["rep"]

    def shards(hidden, train_weight, shard_order):
        piece_rows, tile_cols = train_weight.shape
        cols = tile_cols // n_row
        subs = shard_order.shape[1]
        depth = hidden.shape[1]
        tiles = n_row * subs // 2
        dma = pltpu.SemaphoreType.DMA
        one = dma((n_row,))
        ring = dma((7, 2, n_row))
        served, projected = pl.pallas_call(
            functools.partial(handoff, (n_row, n_col, piece_rows, cols, subs)),
            out_shape=(
                jax.ShapeDtypeStruct((depth, cols), jnp.bfloat16),
                jax.ShapeDtypeStruct((hidden.shape[0], cols), jnp.float32),
            ),
            in_specs=[pl.BlockSpec(memory_space=pltpu.HBM)] * 3,
            out_specs=[pl.BlockSpec(memory_space=pltpu.VMEM)] * 2,
            scratch_shapes=[
                pltpu.SMEM(shard_order.shape, jnp.int32),
                pltpu.VMEM(hidden.shape, jnp.bfloat16),
                pltpu.VMEM((tiles, piece_rows, tile_cols // tiles), jnp.bfloat16),
                pltpu.VMEM((n_row, piece_rows, cols), jnp.bfloat16),
                pltpu.VMEM((n_row, piece_rows, cols), jnp.bfloat16),
                dma((2,)),
                dma,
                pltpu.SemaphoreType.REGULAR((2,)),
                one, one, one, ring, dma((4,)),
            ],
            compiler_params=pltpu.CompilerParams(
                collective_id=0, has_side_effects=True, vmem_limit_bytes=16 * 1024 * 1024
            ),
            name="handoff",
        )(*[pltpu.with_memory_space_constraint(a, pltpu.HBM) for a in (shard_order, hidden, train_weight)])
        chunks = 8
        return pl.pallas_call(
            functools.partial(put_out, chunks),
            out_shape=(
                jax.ShapeDtypeStruct(served.shape, served.dtype),
                jax.ShapeDtypeStruct(projected.shape, projected.dtype),
            ),
            in_specs=[pl.BlockSpec(memory_space=pltpu.VMEM)] * 2,
            out_specs=[pl.BlockSpec(memory_space=pltpu.HBM)] * 2,
            scratch_shapes=[dma((chunks + 1,))],
            compiler_params=pltpu.CompilerParams(vmem_limit_bytes=16 * 1024 * 1024),
            name="put_out",
        )(served, projected)

    return jax.shard_map(
        shards,
        mesh=mesh,
        in_specs=(P("rep", None), P(("rep", "row"), "col"), P()),
        out_specs=(P(None, ("col", "row")), P("rep", ("col", "row"))),
        check_vma=False,
    )
```

```python
import functools

import jax
import jax.numpy as jnp
from jax import lax
from jax.experimental import pallas as pl
from jax.experimental.pallas import tpu as pltpu
from jax.sharding import PartitionSpec as P

MESH = pl.DeviceIdType.MESH
UP, DOWN = 0, 1
STEP = {UP: 1, DOWN: -1}


def handoff(
    sizes, order_hbm, hidden_hbm, tile_hbm, served, projected,
    order, hidden, tile, pieces, relayed, local_sem, tile_sem, ready,
    row_recv, out_recv, on_recv, z_recv, fourth_recv, sent,
):
    n, n_x, piece_rows, cols, subs = sizes
    half_rows = n * piece_rows
    place_rows = 2 * half_rows
    lanes = 2 * cols // subs
    x_los = n_x // 2
    col = lax.axis_index("col")
    row = lax.axis_index("row")
    rep = lax.axis_index("rep")
    z, half = rep // 2, rep % 2
    x = half * x_los + col // 2

    load_order = pltpu.make_async_copy(order_hbm, order, local_sem.at[0])
    load_hidden = pltpu.make_async_copy(hidden_hbm, hidden, local_sem.at[1])
    load_tile = [
        pltpu.make_async_copy(tile_hbm.at[:, i * lanes : (i + 1) * lanes], tile.at[i], tile_sem)
        for i in range(tile.shape[0])
    ]
    load_order.start()
    for copy in load_tile:
        copy.start()
    load_hidden.start()

    def row_of(d):
        return (row + d + n) % n

    def rep_of(e, other):
        return (z + e + n) % n * 2 + (half + other) % 2

    def x_device(w):
        far = (x + 2 * w + n_x) % n_x
        return {"col": far % x_los * 2 + col % 2, "rep": z * 2 + far // x_los}

    def z_device(e):
        return {"rep": rep_of(e, 0)}

    def side(d):
        return 1 - 2 * (d // (n // 2))

    barrier = pltpu.get_barrier_semaphore()

    def greet(device):
        pl.semaphore_signal(barrier, inc=1, device_id=device, device_id_type=MESH)

    for d in range(1, n):
        greet({"row": row_of(d)})
    for w in (1, -1):
        greet(x_device(w))

    @pl.when(z < n - 1)
    def _():
        greet(z_device(1))

    @pl.when(z == 0)
    def _():
        greet(z_device(-1))

    load_order.wait()
    pltpu.make_async_copy(tile, tile, tile_sem).wait()
    low = lax.broadcasted_iota(jnp.int32, (piece_rows, lanes), 1) < lanes // 2
    for s in range(n):
        for pair in range(subs // 2):
            a = tile[order[col, 2 * pair, s] * (subs // 2) + pair]
            b = tile[order[col, 2 * pair + 1, s] * (subs // 2) + pair]
            pieces[s, :, pair * lanes : (pair + 1) * lanes] = jnp.where(low, a, b)

    def piece_at(of_rep, of_row):
        return pl.ds(pl.multiple_of(of_rep * half_rows + of_row * piece_rows, 8), piece_rows)

    served[piece_at(rep, row), :] = pieces[row]
    pl.semaphore_wait(barrier, n + 1 + (z + n - 2) // (n - 1) + z // (n - 1))

    @pl.when(z > 0)
    def _():
        pl.semaphore_signal(ready.at[UP], inc=1, device_id=z_device(-1), device_id_type=MESH)

    @pl.when(z == n - 1)
    def _():
        pl.semaphore_signal(ready.at[DOWN], inc=1, device_id=z_device(1), device_id_type=MESH)

    def copy_of(src, dst, send_sem, recv_sem, device):
        return pltpu.make_async_remote_copy(
            src_ref=src, dst_ref=dst, send_sem=send_sem, recv_sem=recv_sem, device_id=device, device_id_type=MESH
        )

    def await_piece(recv_sem, send_sem):
        copy_of(pieces.at[0], relayed.at[0], send_sem, recv_sem, z_device(1)).wait_recv()

    def served_piece(e, other, d):
        return served.at[piece_at(rep_of(e, other), row_of(-d)), :]

    mine = served.at[piece_at(rep, row), :]

    def nth(i):
        return (i % 2 * ((i + 1) // 2) + (1 - i % 2) * (n - i // 2)) % n

    def each(body):
        lax.fori_loop(0, n, lambda i, c: (body(nth(i)), c)[1], 0)

    for i in range(1, n):
        d = nth(i)
        copy_of(pieces.at[row_of(d)], mine, sent.at[0], row_recv.at[d], {"row": row_of(d)}).start()

    def z_sem(way, step, other, d):
        return fourth_recv if step == n // 2 else z_recv.at[3 * way + step - 1, other, d]

    def z_copy(way, step, other, d):
        piece = served_piece(-STEP[way] * (step - 1), other, d)
        sem = sent.at[1 + way] if step == n // 2 else sent.at[0]
        return copy_of(piece, piece, sem, z_sem(way, step, other, d), z_device(STEP[way]))

    def own(ways, fresh):
        def go(d):
            for way in ways:
                z_copy(way, 1, 0, d).start()
            if fresh:
                piece = served_piece(0, 0, d)
                copy_of(piece, relayed.at[d], sent.at[0], out_recv.at[d], x_device(side(d))).start()

        def body(i, c):
            d = nth(i)
            if fresh:
                await_piece(row_recv.at[d], sent.at[0])
            go(d)
            return c

        go(0)
        lax.fori_loop(1, n, body, 0)

    def relay(d):
        await_piece(out_recv.at[d], sent.at[0])
        w = side(d)
        origin = (x - 2 * w + n_x) % n_x // x_los
        at = piece_at(z * 2 + origin, row_of(-d))
        copy_of(relayed.at[d], served.at[at, :], sent.at[0], on_recv.at[d], x_device(w)).start()

    def others(ways, wait):
        def body(d):
            if wait:
                await_piece(on_recv.at[d], sent.at[0])
            for way in ways:
                z_copy(way, 1, 1, d).start()

        each(body)

    def z_await(way, step, other, d):
        await_piece(z_sem(way, step, other, d), sent.at[0])

    def z_pass(way, step, other, d):
        z_await(way, step, other, d)
        z_copy(way, step + 1, other, d).start()

    def pass_on(*moves):
        def body(d):
            for move in moves:
                z_pass(*move, d)

        each(body)

    BOTH = (DOWN, UP)

    far_down = (z > 0) & (z < 5)
    far_up = (z > 2) & (z < 7)

    def pass_third(other):
        def body(d):
            @pl.when(far_down)
            def _():
                z_pass(DOWN, 3, other, d)

            @pl.when(far_up)
            def _():
                z_pass(UP, 3, other, d)

        each(body)

    @pl.when(z == 0)
    def _():
        pl.semaphore_wait(ready.at[UP], 1)
        own((UP,), True)
        each(relay)
        others((UP,), True)
        pl.semaphore_wait(ready.at[DOWN], 1)
        own((DOWN,), False)
        pass_on((DOWN, 1, 0))
        others((DOWN,), False)
        pass_on((DOWN, 1, 1))
        pass_on((DOWN, 2, 0))
        pass_on((UP, 1, 0))
        pass_on((UP, 2, 0))
        pass_on((DOWN, 2, 1))
        pass_on((UP, 1, 1))
        pass_on((UP, 2, 1))

    @pl.when(z > 0)
    def _():
        @pl.when(z == n - 1)
        def _():
            own(BOTH, True)

        @pl.when(z < n - 1)
        def _():
            own((DOWN,), True)
            pl.semaphore_wait(ready.at[UP], 1)
            own((UP,), False)

        def body(d):
            z_pass(DOWN, 1, 0, d)
            relay(d)
            z_pass(UP, 1, 0, d)

        each(body)

        @pl.when(z == 1)
        def _():
            pass_on((DOWN, 2, 0))
            others(BOTH, True)
            pass_on((DOWN, 1, 1), (UP, 1, 1))
            pass_third(0)
            pass_on((DOWN, 2, 1), (UP, 2, 0))
            pass_third(1)
            pass_on((UP, 2, 1))

        @pl.when(z > 1)
        def _():
            pass_on((DOWN, 2, 0), (UP, 2, 0))
            others(BOTH, True)
            pass_on((DOWN, 1, 1), (UP, 1, 1))
            pass_third(0)
            pass_on((DOWN, 2, 1), (UP, 2, 1))
            pass_third(1)

    load_hidden.wait()

    def product(e):
        at = pl.ds(pl.multiple_of((z + e + n) % n * place_rows, 128), place_rows)
        return jnp.dot(hidden[:, at], served[at, :], preferred_element_type=jnp.float32)

    def sent_pieces(sem, count):
        ref = served.at[pl.ds(0, count * piece_rows), :]
        copy_of(ref, ref, sem, sem, z_device(1)).wait_send()

    def all_sent():
        rest = n - 0
        sent_pieces(sent.at[0], 3 * n - 1 + 6 * (n + rest))
        for way, far in ((DOWN, far_down), (UP, far_up)):

            @pl.when(far)
            def _():
                sent_pieces(sent.at[1 + way], n + rest)

    def third_here(way, far):
        @pl.when(jnp.logical_not(far))
        def _():
            for other in (0, 1):
                each(functools.partial(z_await, way, 3, other))

    projected[...] = product(0)

    def add(e, c):
        projected[...] += product(e)
        return c

    lax.fori_loop(1, 3, lambda e, c: add(n - e, add(e, c)), 0)
    third_here(DOWN, far_down)
    projected[...] += product(3)

    fourth = served.at[pl.ds(0, 2 * half_rows), :]
    copy_of(fourth, fourth, sent.at[0], fourth_recv, z_device(1)).wait_recv()
    projected[...] += product(4)
    third_here(UP, far_up)
    projected[...] += product(-3)
    all_sent()


def put_out(chunks, served, projected, served_out, projected_out, sem):
    rows = served.shape[0] // chunks
    copies = [pltpu.make_async_copy(projected, projected_out, sem.at[chunks])] + [
        pltpu.make_async_copy(served.at[pl.ds(i * rows, rows), :], served_out.at[pl.ds(i * rows, rows), :], sem.at[i])
        for i in range(chunks)
    ]
    for copy in copies:
        copy.start()
    for copy in copies:
        copy.wait()


def solution(mesh):
    n_row, n_col, n_rep = mesh.shape["row"], mesh.shape["col"], mesh.shape["rep"]

    def shards(hidden, train_weight, shard_order):
        piece_rows, tile_cols = train_weight.shape
        cols = tile_cols // n_row
        subs = shard_order.shape[1]
        depth = hidden.shape[1]
        tiles = n_row * subs // 2
        dma = pltpu.SemaphoreType.DMA
        one = dma((n_row,))
        ring = dma((6, 2, n_row))
        served, projected = pl.pallas_call(
            functools.partial(handoff, (n_row, n_col, piece_rows, cols, subs)),
            out_shape=(
                jax.ShapeDtypeStruct((depth, cols), jnp.bfloat16),
                jax.ShapeDtypeStruct((hidden.shape[0], cols), jnp.float32),
            ),
            in_specs=[pl.BlockSpec(memory_space=pltpu.HBM)] * 3,
            out_specs=[pl.BlockSpec(memory_space=pltpu.VMEM)] * 2,
            scratch_shapes=[
                pltpu.SMEM(shard_order.shape, jnp.int32),
                pltpu.VMEM(hidden.shape, jnp.bfloat16),
                pltpu.VMEM((tiles, piece_rows, tile_cols // tiles), jnp.bfloat16),
                pltpu.VMEM((n_row, piece_rows, cols), jnp.bfloat16),
                pltpu.VMEM((n_row, piece_rows, cols), jnp.bfloat16),
                dma((2,)),
                dma,
                pltpu.SemaphoreType.REGULAR((2,)),
                one, one, one, ring, dma, dma((3,)),
            ],
            compiler_params=pltpu.CompilerParams(
                collective_id=0, has_side_effects=True, vmem_limit_bytes=16 * 1024 * 1024
            ),
            name="handoff",
        )(*[pltpu.with_memory_space_constraint(a, pltpu.HBM) for a in (shard_order, hidden, train_weight)])
        chunks = 8
        return pl.pallas_call(
            functools.partial(put_out, chunks),
            out_shape=(
                jax.ShapeDtypeStruct(served.shape, served.dtype),
                jax.ShapeDtypeStruct(projected.shape, projected.dtype),
            ),
            in_specs=[pl.BlockSpec(memory_space=pltpu.VMEM)] * 2,
            out_specs=[pl.BlockSpec(memory_space=pltpu.HBM)] * 2,
            scratch_shapes=[dma((chunks + 1,))],
            compiler_params=pltpu.CompilerParams(vmem_limit_bytes=16 * 1024 * 1024),
            name="put_out",
        )(served, projected)

    return jax.shard_map(
        shards,
        mesh=mesh,
        in_specs=(P("rep", None), P(("rep", "row"), "col"), P()),
        out_specs=(P(None, ("col", "row")), P("rep", ("col", "row"))),
        check_vma=False,
    )
```
